128 devices in a mesh: rows: 8 (over z, y_hi), snaps: 16 (over x, y_lo, core).
Axes of the slice: x: 4, y: 4 (y_hi: 2, y_lo: 2; y = y_hi * 2 + y_lo), z: 4, core: 2. Of those that a mesh axis runs over, the one named last changes fastest.
Arguments:
- snapshots: float32 [16384, 4096], P('rows', 'snaps'), may hold values from -6 to 6
- weights: float32 [16384], P('rows'), may hold values from 0.3 to 3
- next_bricks: float32 [16384, 4096], P(('rows', 'snaps')), may hold values from -6 to 6
- brick_source: int32 [8, 64], P('rows'), may hold values from 0 to 63, each once within a row
Outputs:
- gram: float32 [4096, 4096], P('rows', 'snaps')
- next_tiles: float32 [16384, 4096], P('rows', 'snaps')
The draws below stay inside these ranges and needn't reach their ends.
Inputs may be any that keep to these rules, and one draw needn't show every extreme that they name: Each row of brick_source is a permutation of 0 to 63.
All inputs are finite; a program needn't handle non-finite values.
Results may differ from the reference program's by a relative error of at most 0.00007.
Values sent between devices are 32-bit elements; how exact they have to be, the bound alone decides.
No kernel may reach another device: no remote copies, remote signals or barrier semaphores. Data moves between devices by JAX's collectives and lax.ppermute only.
A program may use at most 128 MiB of HBM per device.

```python
import math
import jax
import jax.numpy as jnp
from jax import lax

BRICK = 32
S = 4096
M = 16384
BRICKS_DEV = 64
N_ROWS = 8


def level_of(stream_key, extent, shards, low, high):
    factor_of = 1.0
    for position, parts in shards:
        heights = jax.random.uniform(jax.random.fold_in(jax.random.fold_in(stream_key, 6), position), (parts,), jnp.float32, low / len(shards), high / len(shards))
        factor_of = factor_of * jnp.repeat(jnp.exp(heights), extent[position] // parts).reshape((-1,) + (1,) * (len(extent) - 1 - position))
    return factor_of


def normal_values(stream_key, dims, scale, reach, pieces=(), dtype=jnp.bfloat16):
    result = jax.random.normal(stream_key, dims, jnp.float32) * scale
    if len(pieces) > 0:
        result = level_of(stream_key, dims, pieces, -0.22, 0.18) * result
    return jnp.clip(result, min=-reach, max=reach).astype(dtype)


def setup_inputs(seed: int = 0) -> dict:
    key_of = jax.random.split(jax.random.key(seed), 5)
    snapshots = normal_values(key_of[0], (M, S), 1.0, 6.0, ((0, 8), (1, 16)), jnp.float32)
    weights = jnp.clip(jnp.exp(math.log(3.0) - 2.3025851 * jax.random.uniform(key_of[1], (M,), jnp.float32) ** level_of(key_of[1], (M,), ((0, 8),), -0.2, 0.2)), 0.3, 3.0)
    next_bricks = normal_values(key_of[2], (M, S), 1.0, 6.0, ((0, 128),), jnp.float32)
    brick_source = jax.vmap(lambda own: jax.random.permutation(own, BRICKS_DEV))(jax.random.split(key_of[3], N_ROWS)).reshape((N_ROWS, BRICKS_DEV)).astype(jnp.int32)
    return dict(snapshots=snapshots, weights=weights, next_bricks=next_bricks, brick_source=brick_source)


def pick_bricks(block, order):
    return jnp.take(block, order, axis=0)

def reference(snapshots, weights, next_bricks, brick_source):
    weighted = snapshots * weights[:, None]
    product = lax.dot_general(snapshots, weighted, (((0,), (0,)), ((), ())), precision=lax.Precision.HIGHEST, preferred_element_type=jnp.float32)
    gram = product / jnp.float32(math.sqrt(M))
    blocks = next_bricks.reshape(N_ROWS, BRICKS_DEV, BRICK, S)
    moved = jax.vmap(pick_bricks)(blocks, brick_source)
    next_tiles = moved.reshape(M, S)
    return (gram, next_tiles)
```

```python
import math

import jax
import jax.numpy as jnp
import numpy as np
from jax import lax
from jax.sharding import Mesh
from jax.sharding import PartitionSpec as P

BRICK = 32
AXES = ("z", "yh", "x", "yl", "c")
SIZES = (4, 2, 4, 2, 2)
ROWS = ("z", "yh")
SNAPS = ("x", "yl", "c")


def send(value, target):
    pairs = []
    for source in np.ndindex(*SIZES):
        dest = target(*source)
        if dest is not None:
            dest = tuple(d % n for d, n in zip(dest, SIZES))
            pairs.append((np.ravel_multi_index(source, SIZES), np.ravel_multi_index(dest, SIZES)))
    return lax.ppermute(value, AXES, [(int(a), int(b)) for a, b in pairs])


def dot(left, right):
    return lax.dot_general(
        left,
        right,
        (((0,), (0,)), ((), ())),
        precision=lax.Precision.HIGH,
        preferred_element_type=jnp.float32,
    )


def sum_over_z(blocks, dests, e):
    slot = [blocks[dests.index(d)] if d in dests else blocks[0] for d in range(4)]
    stack = jnp.stack(slot)
    pick = lambda j: lax.dynamic_index_in_dim(stack, (e + j) % 4, 0, keepdims=False)
    total = pick(0)
    for j in (1, 3, 2):
        total = total + send(
            pick(j),
            lambda z, yh, x, yl, c: (z + j, yh, x, yl, c) if (z + j - x) % 4 in dests else None,
        )
    return total


def gram_tile(own, weights):
    z, yh, x, yl, c = (lax.axis_index(a) for a in AXES)
    e = (z - x) % 4
    f = (yh + yl) % 2

    swap = lambda v: send(v, lambda z, yh, x, yl, c: (z, yh, x, yl, 1 - c))
    ahead = send(own, lambda z, yh, x, yl, c: (z, yh, x - 1, yl, c))
    behind = send(own, lambda z, yh, x, yl, c: (z, yh, x + 1, yl, c))
    both = lambda v: jnp.concatenate([v, swap(v)], axis=1)
    own2, ahead2, behind2 = both(own), both(ahead), both(behind)
    diag = send(ahead, lambda z, yh, x, yl, c: (z, yh, x, 1 - yl, c))

    w = weights[:, None]
    early = [dot(own2, own * w), dot(own2, ahead * w), dot(behind2, ahead * w)]
    late = [dot(ahead2, diag * w), dot(own2, diag * w), dot(behind2, diag * w)]

    dests = (0, 1, 3)
    early = sum_over_z(early, dests, e)
    late = sum_over_z(late, dests, e)

    early = early + send(
        early, lambda z, yh, x, yl, c: (z, 1 - yh, x, yl, c) if yh != yl and (z - x) % 4 != 2 else None
    )
    late = late + send(
        late, lambda z, yh, x, yl, c: (z, 1 - yh, x, yl, c) if yh == yl and (z - x) % 4 != 2 else None
    )

    def early_place(z, yh, x, yl, c):
        e = (z - x) % 4
        if yh != yl or e not in (1, 3):
            return None
        return (x, yl, x + 1, yl, c) if e == 1 else (x - 1, yl, x + 1, yl, c)

    def late_place(z, yh, x, yl, c):
        e = (z - x) % 4
        if yh == yl or e not in (0, 1, 3):
            return None
        return ({0: x + 1, 1: x, 3: x - 1}[e], yl, x + 1, 1 - yl, c)

    moved = send(early, early_place) + send(late, late_place)
    mine = jnp.where(f == 0, early, late)
    half = mine.shape[0] // 2
    turned = jnp.concatenate([mine[:half].T, swap(mine[half:]).T], axis=0)
    block = jnp.where(e == 1, turned, jnp.where((e == 0) & (f == 0), mine, moved))
    block = jnp.where(c == 0, block, jnp.roll(block, half, axis=0))
    return block


def per_device(snapshots, weights, next_bricks, brick_source):
    width = snapshots.shape[1]
    scale = jnp.float32(math.sqrt(snapshots.shape[0] * lax.axis_size(ROWS)))
    gram = gram_tile(snapshots, weights) / scale
    arrived = lax.all_to_all(next_bricks, SNAPS, split_axis=1, concat_axis=0, tiled=True)
    bricks = arrived.reshape(-1, BRICK, width)
    next_tiles = jnp.take(bricks, brick_source[0], axis=0).reshape(-1, width)
    return (gram, next_tiles)


def solution(mesh):
    torus = Mesh(mesh.devices.reshape(SIZES), AXES)
    in_specs = (P(ROWS, SNAPS), P(ROWS), P(ROWS + SNAPS, None), P(ROWS, None))
    out_specs = (P(ROWS, SNAPS), P(ROWS, SNAPS))
    return jax.shard_map(
        per_device, mesh=torus, in_specs=in_specs, out_specs=out_specs, check_vma=False
    )
```
